32 devices in a mesh: batch: 1 (over z), z: 4 (over y), y: 4 (over x), x: 2 (over core).
Axes of the slice: x: 4, y: 4, z: 1, core: 2. Of those that a mesh axis runs over, the one named last changes fastest.
The devices are a block of a 4x4x8 slice.
Arguments:
- volume: bfloat16 [32, 128, 256, 256], P('batch', 'x', 'y', 'z')
- filter_taps: float32 [3, 3, 17], replicated
- mix_w: bfloat16 [3, 32, 32], replicated
- mix_bias: float32 [3, 32], replicated
Outputs:
- output: bfloat16 [32, 128, 256, 256], P('batch', 'x', 'y', 'z')
All inputs are finite; a program needn't handle non-finite values.
Results may differ from the reference program's by a relative error of at most 0.00526.
Values are sent between devices in bfloat16 or wider.
A program may use at most 768 MiB of HBM per device.

```python
import jax
import jax.numpy as jnp
from jax import lax

CHANNELS = 32
KERNEL = 17
LAYERS = 3
GRID_X = 128
GRID_Y = 256
GRID_Z = 256
HALF = (KERNEL - 1) // 2


def setup_inputs(seed: int = 0, part: int = 0) -> dict:
    vol_key = jax.random.fold_in(jax.random.key(seed), part)
    key_mag, key_sign, key_mix, key_bias = jax.random.split(jax.random.key(seed + 1), 4)
    volume = jax.random.normal(vol_key, (CHANNELS, GRID_X, GRID_Y, GRID_Z), jnp.float32)
    tap_mag = jax.random.uniform(key_mag, (LAYERS, 3, KERNEL), jnp.float32, 0.5, 1.5)
    tap_sign = jax.random.bernoulli(key_sign, 0.5, (LAYERS, 3, KERNEL)).astype(jnp.float32) * 2.0 - 1.0
    filter_taps = tap_sign * tap_mag * (KERNEL ** -0.5)
    mix_w = jax.random.normal(key_mix, (LAYERS, CHANNELS, CHANNELS), jnp.float32) * (CHANNELS ** -0.5)
    mix_bias = 0.5 * jax.random.normal(key_bias, (LAYERS, CHANNELS), jnp.float32)
    return {"volume": volume.astype(jnp.bfloat16), "filter_taps": filter_taps, "mix_w": mix_w.astype(jnp.bfloat16), "mix_bias": mix_bias}


def axis_pass(chan_vol, taps_row, axis_pos):
    pad_widths = tuple((HALF, HALF) if dim_idx == axis_pos else (0, 0) for dim_idx in range(3))
    padded = jnp.pad(chan_vol.astype(jnp.float32), pad_widths)
    length = chan_vol.shape[axis_pos]
    accum_sum = jnp.zeros(chan_vol.shape, jnp.float32)
    for offset in range(KERNEL):
        accum_sum = accum_sum + taps_row[offset] * lax.slice_in_dim(padded, offset, offset + length, axis=axis_pos)
    return accum_sum.astype(jnp.bfloat16)


def reference(volume, filter_taps, mix_w, mix_bias):
    taps_b = filter_taps.astype(jnp.bfloat16).astype(jnp.float32)

    def layer_step(carry_vol, layer_in):
        layer_taps, layer_w, layer_b = layer_in

        def channel_filter(chan_vol):
            staged = axis_pass(chan_vol, layer_taps[0], 0)
            staged = axis_pass(staged, layer_taps[1], 1)
            return axis_pass(staged, layer_taps[2], 2)

        filtered = lax.map(channel_filter, carry_vol)
        mixed_out = jnp.dot(layer_w.T, filtered.reshape(CHANNELS, -1), preferred_element_type=jnp.float32)
        activated = jax.nn.gelu(mixed_out + layer_b[:, None], approximate=False)
        new_vol = (carry_vol.astype(jnp.float32) + activated.reshape(carry_vol.shape)).astype(jnp.bfloat16)
        return new_vol, None

    final_vol, _ = lax.scan(layer_step, volume, (taps_b, mix_w, mix_bias))
    return final_vol
```

```python
import jax
import jax.numpy as jnp
from jax import lax
from jax.experimental import pallas as pl
from jax.experimental.pallas import tpu as pltpu
from jax.sharding import PartitionSpec as P

BF = jnp.bfloat16
F32 = jnp.float32
SLAB = 16
JH = 2
SQRT_HALF = 0.7071067811865476


def lane_iota(shape):
    return lax.broadcasted_iota(jnp.int32, shape, len(shape) - 1)


def pick_taps(index, valid, taps):
    index = jnp.where(valid, index, -1)
    out = jnp.zeros((taps.shape[0],) + index.shape, F32)
    for t in range(taps.shape[1]):
        out = jnp.where(index[None] == t, taps[:, t][:, None, None], out)
    return out.astype(BF)


def grid2(rows, cols):
    return (lax.broadcasted_iota(jnp.int32, (rows, cols), 0), lax.broadcasted_iota(jnp.int32, (rows, cols), 1))


def x_table(taps, last):
    r, q = grid2(128, 256)
    i_out, i_in = r // 8, q // 8
    if last:
        i_in = jnp.where(i_in >= 24, 55 - i_in, i_in)
    t = i_in - i_out
    return pick_taps(t, (t >= 0) & (t <= 16) & (r % 8 == q % 8), taps)


def y_table(taps):
    r, q = grid2(128, 256)
    t = (q // 64) * 8 + q % 8 - (r // 64) * 8 - r % 8
    return pick_taps(t, (t >= 0) & (t <= 16) & ((r // 8) % 8 == (q // 8) % 8), taps)


def z_tables(taps):
    m, n = grid2(256, 256)
    t = m % 64 - n % 64 + 8
    tables = [pick_taps(t, (t >= 0) & (t <= 16) & (m // 64 == n // 64), taps)]
    for v in range(4):
        k = jnp.where(m < 128, -8, 64) + m % 8
        t = k - n % 64 + 8
        ok = ((m // 64) % 2 == (n // 64) % 2) & ((m // 8) % 8 == 2 * v + n // 128)
        tables.append(pick_taps(t, (t >= 0) & (t <= 16) & ok, taps))
    return jnp.stack(tables, axis=1)


def mix_table(mix_w):
    r, q = grid2(256, 32)
    spread = (r // 8 == q).astype(BF)
    full = jnp.einsum("rd,lcd,qc->lrq", spread, mix_w, spread, preferred_element_type=F32)
    r, q = grid2(256, 256)
    return jnp.where((r % 8 == q % 8)[None], full, 0.0).astype(BF)


def cost(flops):
    return pl.CostEstimate(flops=flops, bytes_accessed=8 << 20, transcendentals=0)


def params():
    return pltpu.CompilerParams(vmem_limit_bytes=60 << 20)


def relayout_in(volume, xi):
    C, I, J, K = volume.shape
    n_slab, cb = I // SLAB, 8

    def body(xi_ref, x_ref, o_ref):
        flip = xi_ref[0]
        for tp in range(SLAB // 2):
            rows = []
            for t in (2 * tp, 2 * tp + 1):
                a = x_ref[:, jnp.where(flip == 1, SLAB - 1 - t, t)].astype(F32)
                a = jnp.concatenate([a[:, : J // 2], a[:, J // 2 :]], axis=2)
                rows.append(a.reshape(cb, 4, 8, 128))
            o_ref[:, :, 16 * tp : 16 * tp + 16, :] = jnp.concatenate(rows, axis=2).astype(BF)

    return pl.pallas_call(
        body,
        grid_spec=pltpu.PrefetchScalarGridSpec(
            num_scalar_prefetch=1,
            grid=(n_slab, C // cb),
            in_specs=[pl.BlockSpec((cb, SLAB, J, K), lambda s, g, f: (g, jnp.where(f[0] == 1, n_slab - 1 - s, s), 0, 0))],
            out_specs=pl.BlockSpec((cb, 4, SLAB * 8, 128), lambda s, g, f: (g, 0, s, 0)),
        ),
        out_shape=jax.ShapeDtypeStruct((C, 4, I * 8, 128), BF),
        compiler_params=params(),
        cost_estimate=cost(1 << 24),
        name="relayout_in",
    )(xi, volume)


def relayout_out(vol, xi, shape):
    C, I, J, K = shape
    cb = 2

    def body(xi_ref, v_ref, o_ref):
        flip = xi_ref[0]
        for tp in range(I // 2):
            a = v_ref[:, :, 16 * tp : 16 * tp + 16, :].astype(F32)
            for u in range(2):
                t = 2 * tp + u
                b = a[:, :, 8 * u : 8 * u + 8, :].reshape(cb, 32, 128)
                b = jnp.concatenate([b[:, :, :64], b[:, :, 64:]], axis=1).astype(BF)
                o_ref[:, jnp.where(flip == 1, I - 1 - t, t)] = b

    return pl.pallas_call(
        body,
        grid_spec=pltpu.PrefetchScalarGridSpec(
            num_scalar_prefetch=1,
            grid=(C // cb,),
            in_specs=[pl.BlockSpec((cb, 4, I * 8, 128), lambda g, f: (g, 0, 0, 0))],
            out_specs=pl.BlockSpec((cb, I, J, K), lambda g, f: (g, 0, 0, 0)),
        ),
        out_shape=jax.ShapeDtypeStruct(shape, BF),
        compiler_params=params(),
        cost_estimate=cost(1 << 26),
        name="relayout_out",
    )(xi, vol)


def x_slab(a, vol, row0, u1, up, dn, C):
    per = 2

    def step(it, _):
        low = lane_iota((128, 128)) < 64
        for q in range(per):
            pair = it * per + q
            ends = []
            for c in (2 * pair, 2 * pair + 1):
                got = []
                for jp in range(2):
                    cols = [vol[c, 2 * jp + b, pl.ds(row0, 256), :] for b in range(2)]
                    u = jnp.dot(a, jnp.concatenate(cols, axis=1), preferred_element_type=F32)
                    u1[c, 2 * jp] = u[:, :128].astype(BF)
                    u1[c, 2 * jp + 1] = u[:, 128:].astype(BF)
                    got.append(u[:, :128] if jp == 0 else u[:, 128:])
                ends.append(got)
            up[pair] = jnp.where(low, pltpu.roll(ends[0][1], 64, 1), ends[1][1]).astype(BF)
            dn[pair] = jnp.where(low, ends[0][0], pltpu.roll(ends[1][0], 64, 1)).astype(BF)
        return 0

    lax.fori_loop(0, C // 2 // per, step, 0)


def y_slab(a, u_ref, b_ref, t_ref, o_ref, up_ref, dn_ref, C):
    def step(pair, _):
        low = lane_iota((128, 128)) < 64
        slot = (lane_iota((2, 16, 128)) % 64) // 8
        c0, c1 = 2 * pair, 2 * pair + 1
        b, t = b_ref[pair].astype(F32), t_ref[pair].astype(F32)
        first = [u_ref[c, 0].astype(F32) for c in (c0, c1)]
        final = [u_ref[c, 3].astype(F32) for c in (c0, c1)]
        lead = [
            jnp.where(low, b, pltpu.roll(final[0], 64, 1)).astype(BF),
            pltpu.roll(jnp.where(low, final[1], b), 64, 1).astype(BF),
        ]
        tail = [
            pltpu.roll(jnp.where(low, t, first[0]), 64, 1).astype(BF),
            jnp.where(low, pltpu.roll(first[1], 64, 1), t).astype(BF),
        ]
        out_rows = pl.ds(pl.multiple_of(16 * pair, 16), 16)
        for g in range(2):
            rows = slice(64 * g, 64 * g + 64)
            for w in range(2):
                cols = []
                for n, c in enumerate((c0, c1)):
                    own = [u_ref[c, jb, rows, :] for jb in range(1, 3)]
                    if w == 0:
                        blocks = [lead[n][rows], u_ref[c, 0, rows, :]] + own
                    else:
                        blocks = own + [u_ref[c, 3, rows, :], tail[n][rows]]
                    cols.append(jnp.concatenate(blocks, axis=0))
                out = jnp.dot(a, jnp.concatenate(cols, axis=1), preferred_element_type=F32)
                out = out.reshape(2, 8, 8, 256)
                out = jnp.concatenate([out[..., :128], out[..., 128:]], axis=2)
                o_ref[2 * w : 2 * w + 2, 8 * g : 8 * g + 8, out_rows, :] = out.astype(BF)
                up = dn = None
                for i in range(8):
                    piece = out[:, i].reshape(32, 128)
                    ru = pltpu.roll(piece, (8 * i + 72) % 128, 1).reshape(2, 16, 128)
                    rd = (piece if i == 0 else pltpu.roll(piece, 8 * i, 1)).reshape(2, 16, 128)
                    up = ru if up is None else jnp.where(slot == i, ru, up)
                    dn = rd if dn is None else jnp.where(slot == i, rd, dn)
                up_ref[2 * w : 2 * w + 2, g, out_rows, :] = up.astype(BF)
                dn_ref[2 * w : 2 * w + 2, g, out_rows, :] = dn.astype(BF)
        return 0

    lax.fori_loop(0, C // 2, step, 0)


def z_slab(z_ref, w_ref, bias_ref, u_ref, b_ref, t_ref, vol, row0, C):
    def step(g, _):
        jb, hi = g // 2, g % 2
        w = w_ref[...]
        bias = bias_ref[...].reshape(C, 8, 128)
        bias = jnp.concatenate([bias, bias], axis=1)
        halo = jnp.concatenate([b_ref[jb, hi], t_ref[jb, hi]], axis=1)
        for p in range(4):
            lhs = jnp.concatenate([u_ref[jb, 8 * hi + 2 * p], u_ref[jb, 8 * hi + 2 * p + 1]], axis=1)
            u3 = jnp.dot(lhs, z_ref[0], preferred_element_type=F32)
            u3 = u3 + jnp.dot(halo, z_ref[1 + p], preferred_element_type=F32)
            m = jnp.dot(w, u3.astype(BF), preferred_element_type=F32).reshape(C, 8, 256)
            m = jnp.concatenate([m[..., :128], m[..., 128:]], axis=1) + bias
            gelu = 0.5 * m * (1.0 + lax.erf(m * SQRT_HALF))
            rows = pl.ds(pl.multiple_of(row0 + 64 * hi + 16 * p, 16), 16)
            v = vol[:, jb, rows, :].astype(F32)
            vol[:, jb, rows, :] = (v + gelu).astype(BF)
        return 0

    lax.fori_loop(0, 8, step, 0)


def fused_layers(v_in, xt, yt, zt, mt, bt, ny, nz):
    C, rows = v_in.shape[0], v_in.shape[2]
    L = xt.shape[0]
    S = rows // 128
    N = L * S
    R = 4
    edge = 64 + rows

    def body(vin, ax, ay, az, am, ab, vout, vol, far, u1, u2, ysend, yrecv, zsend, zrecv,
             in_sem, out_sem, far_ss, far_rs, ys_sem, yr_sem, zs_sem, zr_sem):
        xi, yi, zi = (lax.axis_index(a) for a in ("x", "y", "z"))

        def remote(src, dst, ss, rs, axis, idx):
            return pltpu.make_async_remote_copy(
                src_ref=src, dst_ref=dst, send_sem=ss, recv_sem=rs, device_id={axis: idx}, device_id_type=pl.DeviceIdType.MESH
            )

        def ports(axis, pos, count):
            return ((pos < count - 1, pos + 1, pos > 0), (pos > 0, pos - 1, pos < count - 1))

        def link(axis, pos, count, send, recv, ss, rs):
            info = ports(axis, pos, count)

            def copy(d, n):
                a, b = n % 2, n % R
                return remote(send.at[d, a], recv.at[d, b], ss.at[d, a], rs.at[d, b], axis, info[d][1])

            def start(n):
                for d in range(2):
                    @pl.when(info[d][0])
                    def _():
                        copy(d, n).start()

            def wait_send(n):
                for d in range(2):
                    @pl.when(info[d][0])
                    def _():
                        copy(d, n).wait_send()

            def wait_recv(n):
                for d in range(2):
                    @pl.when(info[d][2])
                    def _():
                        copy(d, n).wait_recv()

            return start, wait_send, wait_recv

        y_start, y_wait_send, y_wait_recv = link("y", yi, ny, ysend, yrecv, ys_sem, yr_sem)
        z_start, z_wait_send, z_wait_recv = link("z", zi, nz, zsend, zrecv, zs_sem, zr_sem)

        def far_copy(l):
            a = l % 2
            return remote(vol.at[:, :, pl.ds(edge - 64, 64), :], far.at[a], far_ss.at[a], far_rs.at[a], "x", 1 - xi)

        def in_copy(s):
            return pltpu.make_async_copy(vin.at[:, :, pl.ds(128 * s, 128), :], vol.at[:, :, pl.ds(64 + 128 * s, 128), :], in_sem.at[s])

        def out_copy(s):
            at = pl.multiple_of(128 * s, 128)
            return pltpu.make_async_copy(vol.at[:, :, pl.ds(64 + at, 128), :], vout.at[:, :, pl.ds(at, 128), :], out_sem.at[s])

        for s in range(S):
            in_copy(s).start()
        barrier = pltpu.get_barrier_semaphore()
        pl.semaphore_signal(barrier, inc=1, device_id={"x": 1 - xi}, device_id_type=pl.DeviceIdType.MESH)
        for axis, pos, count in (("y", yi, ny), ("z", zi, nz)):
            for ok, idx, _ in ports(axis, pos, count):
                @pl.when(ok)
                def _():
                    pl.semaphore_signal(barrier, inc=1, device_id={axis: idx}, device_id_type=pl.DeviceIdType.MESH)
        greet = 1
        for pos, count in ((yi, ny), (zi, nz)):
            greet = greet + (pos > 0).astype(jnp.int32) + (pos < count - 1).astype(jnp.int32)
        pl.semaphore_wait(barrier, greet)

        def zero_margin(c, _):
            for jb in range(4):
                vol[c, jb, 0:64, :] = jnp.zeros((64, 128), BF)
            return 0

        lax.fori_loop(0, C, zero_margin, 0)
        for recv, pos, count in ((yrecv, yi, ny), (zrecv, zi, nz)):
            for d, alone in ((0, pos == 0), (1, pos == count - 1)):
                @pl.when(alone)
                def _():
                    def zero(r, _):
                        for j in range(recv.shape[2]):
                            recv[d, r, j] = jnp.zeros(recv.shape[3:], BF)
                        return 0

                    lax.fori_loop(0, R, zero, 0)

        def stage(n, _):
            @pl.when(n < N)
            def _():
                l, s = n // S, n % S

                @pl.when(n == 0)
                def _():
                    in_copy(0).wait()
                    in_copy(1).wait()

                @pl.when(n == 1)
                def _():
                    for q in range(2, S):
                        in_copy(q).wait()
                    far_copy(0).start()

                @pl.when(s == S - 1)
                def _():
                    far_copy(l).wait()

                    def bring(c, _):
                        for jb in range(4):
                            vol[c, jb, edge : edge + 64, :] = far[l % 2, c, jb]
                        return 0

                    lax.fori_loop(0, C, bring, 0)

                @pl.when(n >= 2)
                def _():
                    y_wait_send(n - 2)

                a = ax[l, (s == S - 1).astype(jnp.int32)]
                x_slab(a, vol, pl.multiple_of(128 * s, 128), u1.at[n % 2], ysend.at[0, n % 2], ysend.at[1, n % 2], C)
                y_start(n)

            @pl.when((n >= 1) & (n <= N))
            def _():
                m = n - 1
                y_wait_recv(m)

                @pl.when(m >= 2)
                def _():
                    z_wait_send(m - 2)

                y_slab(ay[m // S], u1.at[m % 2], yrecv.at[0, m % R], yrecv.at[1, m % R], u2.at[m % 2],
                       zsend.at[0, m % 2], zsend.at[1, m % 2], C)
                z_start(m)

            @pl.when(n >= 2)
            def _():
                m = n - 2
                l, s = m // S, m % S
                z_wait_recv(m)
                z_slab(az.at[l], am.at[l], ab.at[l], u2.at[m % 2], zrecv.at[0, m % R], zrecv.at[1, m % R], vol,
                       64 + 128 * s, C)

                @pl.when((s == S - 1) & (l < L - 1))
                def _():
                    far_copy(l + 1).start()

                @pl.when(l == L - 1)
                def _():
                    out_copy(s).start()

            return 0

        lax.fori_loop(0, N + 2, stage, 0)
        for n in (N - 2, N - 1):
            y_wait_send(n)
            z_wait_send(n)
        for s in range(S):
            out_copy(s).wait()

    vmem = pl.BlockSpec(memory_space=pltpu.VMEM)
    hbm = pl.BlockSpec(memory_space=pltpu.HBM)
    dma = pltpu.SemaphoreType.DMA
    return pl.pallas_call(
        body,
        in_specs=[hbm] + [vmem] * 5,
        out_specs=hbm,
        out_shape=jax.ShapeDtypeStruct(v_in.shape, BF),
        scratch_shapes=[
            pltpu.VMEM((C, 4, rows + 128, 128), BF),
            pltpu.VMEM((2, C, 4, 64, 128), BF),
            pltpu.VMEM((2, C, 4, 128, 128), BF),
            pltpu.VMEM((2, 4, SLAB, 8 * C, 128), BF),
            pltpu.VMEM((2, 2, C // 2, 128, 128), BF),
            pltpu.VMEM((2, R, C // 2, 128, 128), BF),
            pltpu.VMEM((2, 2, 4, 2, 8 * C, 128), BF),
            pltpu.VMEM((2, R, 4, 2, 8 * C, 128), BF),
            dma((S,)),
            dma((S,)),
            dma((2,)),
            dma((2,)),
            dma((2, 2)),
            dma((2, R)),
            dma((2, 2)),
            dma((2, R)),
        ],
        compiler_params=pltpu.CompilerParams(vmem_limit_bytes=67043328, collective_id=0, has_side_effects=True),
        cost_estimate=cost(1 << 32),
        name="fused_layers",
    )(v_in, xt, yt, zt, mt, bt)


def solution(mesh):
    ny, nz = mesh.shape["y"], mesh.shape["z"]

    def local_layers(volume, filter_taps, mix_w, mix_bias):
        xi = lax.axis_index("x").astype(jnp.int32)
        xi_arr = xi.reshape(1)
        layers = filter_taps.shape[0]
        taps = filter_taps.astype(BF).astype(F32)
        taps_x = jnp.where(xi == 1, taps[:, 0, ::-1], taps[:, 0])
        xt = jnp.stack([x_table(taps_x, False), x_table(taps_x, True)], axis=1)
        yt, zt, mt = y_table(taps[:, 1]), z_tables(taps[:, 2]), mix_table(mix_w)
        bt = jnp.broadcast_to(jnp.repeat(mix_bias, 8, axis=1)[:, :, None], (layers, 256, 128))
        out = fused_layers(relayout_in(volume, xi_arr), xt, yt, zt, mt, bt, ny, nz)
        return relayout_out(out, xi_arr, volume.shape)

    vol_spec = P("batch", "x", "y", "z")
    return jax.shard_map(
        local_layers, mesh=mesh, in_specs=(vol_spec, P(), P(), P()), out_specs=vol_spec, check_vma=False
    )
```

```python
import jax
import jax.numpy as jnp
from jax import lax
from jax.experimental import pallas as pl
from jax.experimental.pallas import tpu as pltpu
from jax.sharding import PartitionSpec as P

BF = jnp.bfloat16
F32 = jnp.float32
SLAB = 16
X_UNROLL, Y_UNROLL = 8, 4
JH = 2
SQRT_TWO = 1.4142135623730951


def lane_iota(shape):
    return lax.broadcasted_iota(jnp.int32, shape, len(shape) - 1)


def pick_taps(index, valid, taps):
    index = jnp.where(valid, index, -1)
    out = jnp.zeros((taps.shape[0],) + index.shape, F32)
    for t in range(taps.shape[1]):
        out = jnp.where(index[None] == t, taps[:, t][:, None, None], out)
    return out.astype(BF)


def grid2(rows, cols):
    return (lax.broadcasted_iota(jnp.int32, (rows, cols), 0), lax.broadcasted_iota(jnp.int32, (rows, cols), 1))


def x_table(taps, last):
    r, q = grid2(128, 256)
    i_out, i_in = r // 8, q // 8
    if last:
        i_in = jnp.where(i_in >= 24, 55 - i_in, i_in)
    t = i_in - i_out
    return pick_taps(t, (t >= 0) & (t <= 16) & (r % 8 == q % 8), taps)


def y_table(taps):
    r, q = grid2(128, 256)
    t = (q // 64) * 8 + q % 8 - (r // 64) * 8 - r % 8
    return pick_taps(t, (t >= 0) & (t <= 16) & ((r // 8) % 8 == (q // 8) % 8), taps)


def z_tables(taps):
    m, n = grid2(256, 256)
    t = m % 64 - n % 64 + 8
    tables = [pick_taps(t, (t >= 0) & (t <= 16) & (m // 64 == n // 64), taps)]
    for v in range(4):
        k = jnp.where(m < 128, -8, 64) + m % 8
        t = k - n % 64 + 8
        ok = ((m // 64) % 2 == (n // 64) % 2) & ((m // 8) % 8 == 2 * v + n // 128)
        tables.append(pick_taps(t, (t >= 0) & (t <= 16) & ok, taps))
    return jnp.stack(tables, axis=1)


def mix_table(mix_w):
    r, q = grid2(256, 32)
    spread = (r // 8 == q).astype(BF)
    full = jnp.einsum("rd,lcd,qc->lrq", spread, mix_w, spread, preferred_element_type=F32)
    r, q = grid2(256, 256)
    return jnp.where((r % 8 == q % 8)[None], 0.5 * full, 0.0).astype(BF)


def cost(flops):
    return pl.CostEstimate(flops=flops, bytes_accessed=8 << 20, transcendentals=0)


def params():
    return pltpu.CompilerParams(vmem_limit_bytes=60 << 20)


def relayout_in(volume, xi):
    C, I, J, K = volume.shape
    n_slab, cb = I // SLAB, 8

    def body(xi_ref, x_ref, o_ref):
        flip = xi_ref[0]
        for tp in range(SLAB // 2):
            rows = []
            for t in (2 * tp, 2 * tp + 1):
                a = x_ref[:, jnp.where(flip == 1, SLAB - 1 - t, t)].astype(F32)
                a = jnp.concatenate([a[:, : J // 2], a[:, J // 2 :]], axis=2)
                rows.append(a.reshape(cb, 4, 8, 128))
            both = jnp.concatenate(rows, axis=2).astype(BF)
            for jb in range(4):
                o_ref[jb, :, 16 * tp : 16 * tp + 16, :] = both[:, jb]

    return pl.pallas_call(
        body,
        grid_spec=pltpu.PrefetchScalarGridSpec(
            num_scalar_prefetch=1,
            grid=(n_slab, C // cb),
            in_specs=[pl.BlockSpec((cb, SLAB, J, K), lambda s, g, f: (g, jnp.where(f[0] == 1, n_slab - 1 - s, s), 0, 0))],
            out_specs=pl.BlockSpec((4, cb, SLAB * 8, 128), lambda s, g, f: (0, g, s, 0)),
        ),
        out_shape=jax.ShapeDtypeStruct((4, C, I * 8, 128), BF),
        compiler_params=params(),
        cost_estimate=cost(1 << 24),
        name="relayout_in",
    )(xi, volume)


def relayout_out(vol, xi, shape):
    C, I, J, K = shape
    cb = 2

    def body(xi_ref, v_ref, o_ref):
        flip = xi_ref[0]
        for tp in range(I // 2):
            a = [v_ref[jb, :, 16 * tp : 16 * tp + 16, :].astype(F32) for jb in range(4)]
            for u in range(2):
                t = 2 * tp + u
                b = jnp.concatenate([q[:, 8 * u : 8 * u + 8, :] for q in a], axis=1)
                b = jnp.concatenate([b[:, :, :64], b[:, :, 64:]], axis=1).astype(BF)
                o_ref[:, jnp.where(flip == 1, I - 1 - t, t)] = b

    return pl.pallas_call(
        body,
        grid_spec=pltpu.PrefetchScalarGridSpec(
            num_scalar_prefetch=1,
            grid=(C // cb,),
            in_specs=[pl.BlockSpec((4, cb, I * 8, 128), lambda g, f: (0, g, 0, 0))],
            out_specs=pl.BlockSpec((cb, I, J, K), lambda g, f: (g, 0, 0, 0)),
        ),
        out_shape=jax.ShapeDtypeStruct(shape, BF),
        compiler_params=params(),
        cost_estimate=cost(1 << 26),
        name="relayout_out",
    )(xi, vol)


def x_slab(a, vol, row0, u1, up, dn, C):
    per = X_UNROLL

    def step(it, _):
        low = lane_iota((128, 128)) < 64
        for q in range(per):
            pair = it * per + q
            ends = []
            for c in (2 * pair, 2 * pair + 1):
                got = []
                for jp in range(2):
                    cols = [vol[2 * jp + b, c, pl.ds(row0, 256), :] for b in range(2)]
                    u = jnp.dot(a, jnp.concatenate(cols, axis=1), preferred_element_type=F32)
                    u = u.astype(BF)
                    u1[c, 2 * jp] = u[:, :128]
                    u1[c, 2 * jp + 1] = u[:, 128:]
                    got.append(u[:, :128] if jp == 0 else u[:, 128:])
                ends.append(got)
            up[pair] = jnp.where(low, pltpu.roll(ends[0][1], 64, 1), ends[1][1])
            dn[pair] = jnp.where(low, ends[0][0], pltpu.roll(ends[1][0], 64, 1))
        return 0

    lax.fori_loop(0, C // 2 // per, step, 0)


def y_slab(a, u_ref, b_ref, t_ref, o_ref, up_ref, dn_ref, C):
    def one(pair):
        low = lane_iota((128, 128)) < 64
        slot = (lane_iota((16, 128)) % 64) // 8
        c0, c1 = 2 * pair, 2 * pair + 1
        b, t = b_ref[pair], t_ref[pair]
        first = [u_ref[c, 0] for c in (c0, c1)]
        final = [u_ref[c, 3] for c in (c0, c1)]
        lead = [
            jnp.where(low, b, pltpu.roll(final[0], 64, 1)),
            pltpu.roll(jnp.where(low, final[1], b), 64, 1),
        ]
        tail = [
            pltpu.roll(jnp.where(low, t, first[0]), 64, 1),
            jnp.where(low, pltpu.roll(first[1], 64, 1), t),
        ]
        out_rows = pl.ds(pl.multiple_of(16 * pair, 16), 16)
        for g in range(2):
            rows = slice(64 * g, 64 * g + 64)
            for w in range(2):
                cols = []
                for n, c in enumerate((c0, c1)):
                    own = [u_ref[c, jb, rows, :] for jb in range(1, 3)]
                    if w == 0:
                        blocks = [lead[n][rows], u_ref[c, 0, rows, :]] + own
                    else:
                        blocks = own + [u_ref[c, 3, rows, :], tail[n][rows]]
                    cols.append(jnp.concatenate(blocks, axis=0))
                out = jnp.dot(a, jnp.concatenate(cols, axis=1), preferred_element_type=F32)
                out = out.reshape(2, 8, 8, 256)
                out = jnp.concatenate([out[..., :128], out[..., 128:]], axis=2).astype(BF)
                o_ref[2 * w : 2 * w + 2, 8 * g : 8 * g + 8, out_rows, :] = out
                for e in range(2):
                    up = dn = None
                    for i in range(8):
                        ru = pltpu.roll(out[e, i], (8 * i + 72) % 128, 1)
                        rd = out[e, i] if i == 0 else pltpu.roll(out[e, i], 8 * i, 1)
                        up = ru if up is None else jnp.where(slot == i, ru, up)
                        dn = rd if dn is None else jnp.where(slot == i, rd, dn)
                    up_ref[2 * w + e, g, out_rows, :] = up
                    dn_ref[2 * w + e, g, out_rows, :] = dn

    def step(it, _):
        for q in range(Y_UNROLL):
            one(it * Y_UNROLL + q)
        return 0

    lax.fori_loop(0, C // 2 // Y_UNROLL, step, 0)


def z_slab(z_ref, w_ref, bias_ref, u_ref, b_ref, t_ref, vol, row0, u3_ref, C):
    def z_pair(jb, ip):
        lhs = jnp.concatenate([u_ref[jb, 2 * ip + q, : 8 * C, :] for q in range(2)], axis=1)
        halo = jnp.concatenate([b_ref[jb, ip // 4], t_ref[jb, ip // 4]], axis=1)
        u3 = jnp.dot(lhs, z_ref[0], preferred_element_type=F32)
        u3 = u3 + jnp.dot(halo, z_ref[1 + ip % 4], preferred_element_type=F32)
        return u3.astype(BF)

    u3_ref[...] = z_pair(0, 0)

    def step(jb, _):
        u3 = u3_ref[...]
        for ip in range(8):
            ahead = z_pair(jb, ip + 1) if ip < 7 else z_pair(jnp.minimum(jb + 1, 3), 0)
            bias = bias_ref[...].reshape(C, 8, 128)
            m = jnp.dot(w_ref[...], u3, preferred_element_type=F32).reshape(C, 8, 256)
            m = jnp.concatenate([m[..., :128] + bias, m[..., 128:] + bias], axis=1)
            gelu = m + m * lax.erf(m * SQRT_TWO)
            rows = pl.ds(pl.multiple_of(row0 + 16 * ip, 16), 16)
            v = vol[jb, :, rows, :].astype(F32)
            vol[jb, :, rows, :] = (v + gelu).astype(BF)
            u3 = ahead
        u3_ref[...] = u3
        return 0

    lax.fori_loop(0, 4, step, 0)


def fused_layers(v_in, xt, yt, zt, mt, bt, ny, nz):
    C, rows = v_in.shape[1], v_in.shape[2]
    L = xt.shape[0]
    S = rows // 128
    N = L * S
    R = 4
    edge = 64 + rows

    def body(vin, ax, ay, az, am, ab, vout, vol, far, u1, u2, u3, ysend, yrecv, zsend, zrecv,
             in_sem, out_sem, far_ss, far_rs, ys_sem, yr_sem, zs_sem, zr_sem):
        xi, yi, zi = (lax.axis_index(a) for a in ("x", "y", "z"))

        def remote(src, dst, ss, rs, axis, idx):
            return pltpu.make_async_remote_copy(
                src_ref=src, dst_ref=dst, send_sem=ss, recv_sem=rs, device_id={axis: idx}, device_id_type=pl.DeviceIdType.MESH
            )

        def ports(axis, pos, count):
            return ((pos < count - 1, pos + 1, pos > 0), (pos > 0, pos - 1, pos < count - 1))

        def link(axis, pos, count, send, recv, ss, rs):
            info = ports(axis, pos, count)

            def copy(d, n):
                a, b = n % 2, n % R
                return remote(send.at[d, a], recv.at[d, b], ss.at[d, a], rs.at[d, b], axis, info[d][1])

            def start(n):
                for d in range(2):
                    @pl.when(info[d][0])
                    def _():
                        copy(d, n).start()

            def wait_send(n):
                for d in range(2):
                    @pl.when(info[d][0])
                    def _():
                        copy(d, n).wait_send()

            def wait_recv(n):
                for d in range(2):
                    @pl.when(info[d][2])
                    def _():
                        copy(d, n).wait_recv()

            return start, wait_send, wait_recv

        y_start, y_wait_send, y_wait_recv = link("y", yi, ny, ysend, yrecv, ys_sem, yr_sem)
        z_start, z_wait_send, z_wait_recv = link("z", zi, nz, zsend, zrecv, zs_sem, zr_sem)

        def far_copy(l):
            a = l % 2
            return remote(vol.at[:, :, pl.ds(edge - 64, 64), :], far.at[a], far_ss.at[a], far_rs.at[a], "x", 1 - xi)

        def in_copy(s):
            return pltpu.make_async_copy(vin.at[:, :, pl.ds(128 * s, 128), :], vol.at[:, :, pl.ds(64 + 128 * s, 128), :], in_sem.at[s])

        def out_copy(s):
            at = pl.multiple_of(128 * s, 128)
            return pltpu.make_async_copy(vol.at[:, :, pl.ds(64 + at, 128), :], vout.at[:, :, pl.ds(at, 128), :], out_sem.at[s])

        for s in range(S):
            in_copy(s).start()
        barrier = pltpu.get_barrier_semaphore()
        pl.semaphore_signal(barrier, inc=1, device_id={"x": 1 - xi}, device_id_type=pl.DeviceIdType.MESH)
        for axis, pos, count in (("y", yi, ny), ("z", zi, nz)):
            for ok, idx, _ in ports(axis, pos, count):
                @pl.when(ok)
                def _():
                    pl.semaphore_signal(barrier, inc=1, device_id={axis: idx}, device_id_type=pl.DeviceIdType.MESH)
        greet = 1
        for pos, count in ((yi, ny), (zi, nz)):
            greet = greet + (pos > 0).astype(jnp.int32) + (pos < count - 1).astype(jnp.int32)
        pl.semaphore_wait(barrier, greet)

        def zero_margin(c, _):
            for jb in range(4):
                vol[jb, c, 0:64, :] = jnp.zeros((64, 128), BF)
            return 0

        lax.fori_loop(0, C, zero_margin, 0)
        for recv, pos, count in ((yrecv, yi, ny), (zrecv, zi, nz)):
            for d, alone in ((0, pos == 0), (1, pos == count - 1)):
                @pl.when(alone)
                def _():
                    def zero(r, _):
                        for j in range(recv.shape[2]):
                            recv[d, r, j] = jnp.zeros(recv.shape[3:], BF)
                        return 0

                    lax.fori_loop(0, R, zero, 0)

        def stage(n, _):
            @pl.when(n < N)
            def _():
                l, s = n // S, n % S

                @pl.when(n == 0)
                def _():
                    in_copy(0).wait()
                    in_copy(1).wait()

                @pl.when(n == 1)
                def _():
                    for q in range(2, S):
                        in_copy(q).wait()
                    far_copy(0).start()

                @pl.when(s == S - 1)
                def _():
                    far_copy(l).wait()

                    def bring(c, _):
                        for jb in range(4):
                            vol[jb, c, edge : edge + 64, :] = far[l % 2, jb, c]
                        return 0

                    lax.fori_loop(0, C, bring, 0)

                @pl.when(n >= 2)
                def _():
                    y_wait_send(n - 2)

                a = ax[l, (s == S - 1).astype(jnp.int32)]
                x_slab(a, vol, pl.multiple_of(128 * s, 128), u1.at[n % 2], ysend.at[0, n % 2], ysend.at[1, n % 2], C)
                y_start(n)

            @pl.when((n >= 1) & (n <= N))
            def _():
                m = n - 1
                y_wait_recv(m)

                @pl.when(m >= 2)
                def _():
                    z_wait_send(m - 2)

                y_slab(ay[m // S], u1.at[m % 2], yrecv.at[0, m % R], yrecv.at[1, m % R], u2.at[m % 2],
                       zsend.at[0, m % 2], zsend.at[1, m % 2], C)
                z_start(m)

            @pl.when(n >= 2)
            def _():
                m = n - 2
                l, s = m // S, m % S
                z_wait_recv(m)
                z_slab(az.at[l], am.at[l], ab.at[l], u2.at[m % 2], zrecv.at[0, m % R], zrecv.at[1, m % R], vol,
                       64 + 128 * s, u3, C)

                @pl.when((s == S - 1) & (l < L - 1))
                def _():
                    far_copy(l + 1).start()

                @pl.when(l == L - 1)
                def _():
                    out_copy(s).start()

            return 0

        lax.fori_loop(0, N + 2, stage, 0)
        for n in (N - 2, N - 1):
            y_wait_send(n)
            z_wait_send(n)
        for s in range(S):
            out_copy(s).wait()

    vmem = pl.BlockSpec(memory_space=pltpu.VMEM)
    hbm = pl.BlockSpec(memory_space=pltpu.HBM)
    dma = pltpu.SemaphoreType.DMA
    return pl.pallas_call(
        body,
        in_specs=[hbm] + [vmem] * 5,
        out_specs=hbm,
        out_shape=jax.ShapeDtypeStruct(v_in.shape, BF),
        scratch_shapes=[
            pltpu.VMEM((4, C, rows + 128, 128), BF),
            pltpu.VMEM((2, 4, C, 64, 128), BF),
            pltpu.VMEM((2, C, 4, 128, 128), BF),
            pltpu.VMEM((2, 4, SLAB, 8 * C, 128), BF),
            pltpu.VMEM((8 * C, 256), BF),
            pltpu.VMEM((2, 2, C // 2, 128, 128), BF),
            pltpu.VMEM((2, R, C // 2, 128, 128), BF),
            pltpu.VMEM((2, 2, 4, 2, 8 * C, 128), BF),
            pltpu.VMEM((2, R, 4, 2, 8 * C, 128), BF),
            dma((S,)),
            dma((S,)),
            dma((2,)),
            dma((2,)),
            dma((2, 2)),
            dma((2, R)),
            dma((2, 2)),
            dma((2, R)),
        ],
        compiler_params=pltpu.CompilerParams(vmem_limit_bytes=67043328, collective_id=0, has_side_effects=True),
        cost_estimate=cost(1 << 32),
        name="fused_layers",
    )(v_in, xt, yt, zt, mt, bt)


def solution(mesh):
    ny, nz = mesh.shape["y"], mesh.shape["z"]

    def local_layers(volume, filter_taps, mix_w, mix_bias):
        xi = lax.axis_index("x").astype(jnp.int32)
        xi_arr = xi.reshape(1)
        layers = filter_taps.shape[0]
        taps = filter_taps.astype(BF).astype(F32)
        taps_x = jnp.where(xi == 1, taps[:, 0, ::-1], taps[:, 0])
        xt = jnp.stack([x_table(taps_x, False), x_table(taps_x, True)], axis=1)
        yt, zt, mt = y_table(taps[:, 1]), z_tables(taps[:, 2]), mix_table(mix_w)
        bt = jnp.broadcast_to(jnp.repeat(0.5 * mix_bias, 8, axis=1)[:, :, None], (layers, 256, 128))
        out = fused_layers(relayout_in(volume, xi_arr), xt, yt, zt, mt, bt, ny, nz)
        return relayout_out(out, xi_arr, volume.shape)

    vol_spec = P("batch", "x", "y", "z")
    return jax.shard_map(
        local_layers, mesh=mesh, in_specs=(vol_spec, P(), P(), P()), out_specs=vol_spec, check_vma=False
    )
```

```python
import jax
import jax.numpy as jnp
from jax import lax
from jax.experimental import pallas as pl
from jax.experimental.pallas import tpu as pltpu
from jax.sharding import PartitionSpec as P

BF = jnp.bfloat16
F32 = jnp.float32
SLAB = 16
X_UNROLL, Y_UNROLL = 8, 4
JH = 2
SQRT_TWO = 1.4142135623730951


def lane_iota(shape):
    return lax.broadcasted_iota(jnp.int32, shape, len(shape) - 1)


def iota2(rows, cols, row0=0):
    return lax.broadcasted_iota(jnp.int32, (rows, cols), 0) + row0, lax.broadcasted_iota(jnp.int32, (rows, cols), 1)


def tap_values(taps, row, index, valid, mirrored=None):
    index = jnp.where(valid, index, -1)
    count = taps.shape[1]
    out = jnp.zeros(index.shape, F32)
    for t in range(count):
        src = t if mirrored is None else jnp.where(mirrored, count - 1 - t, t)
        out = jnp.where(index == t, taps[row, src], out)
    return out


def build_x_tables(taps, ax, mirrored):
    span = taps.shape[1]

    def layer(l, _):
        for last in range(2):
            for r0 in range(0, 128, 32):
                r, q = iota2(32, 256, r0)
                i_in = q // 8
                if last:
                    i_in = jnp.where(i_in >= 24, 55 - i_in, i_in)
                t = i_in - r // 8
                ok = (t >= 0) & (t < span) & (r % 8 == q % 8)
                ax[l, last, r0 : r0 + 32, :] = tap_values(taps, 3 * l, t, ok, mirrored).astype(BF)
        return 0

    lax.fori_loop(0, ax.shape[0], layer, 0)


def build_tables(taps, mix_w, bias, ay, az, am, ab):
    C = mix_w.shape[1]
    span = taps.shape[1]

    def layer(l, _):
        for r0 in range(0, 128, 32):
            r, q = iota2(32, 256, r0)
            t = (q // 64) * 8 + q % 8 - (r // 64) * 8 - r % 8
            ok = (t >= 0) & (t < span) & ((r // 8) % 8 == (q // 8) % 8)
            ay[l, r0 : r0 + 32, :] = tap_values(taps, 3 * l + 1, t, ok).astype(BF)
        for k0 in range(0, 64, 32):
            k, n = iota2(32, 256, k0)
            t = k - n % 64 + 8
            base = tap_values(taps, 3 * l + 2, t, (t >= 0) & (t < span))
            for g in range(4):
                az[l, 0, 64 * g + k0 : 64 * g + k0 + 32, :] = jnp.where(n // 64 == g, base, 0.0).astype(BF)
        for v in range(4):
            for r0 in range(0, 256, 64):
                az[l, 1 + v, r0 : r0 + 64, :] = jnp.zeros((64, 256), BF)
        r, n = iota2(16, 256)
        for side in range(2):
            t = r % 8 - n % 64 + 72 * side
            base = tap_values(taps, 3 * l + 2, t, (t >= 0) & (t < span) & (r // 8 == n // 128))
            for jh in range(2):
                block = jnp.where((n // 64) % 2 == jh, base, 0.0).astype(BF)
                for v in range(4):
                    r0 = 128 * side + 64 * jh + 16 * v
                    az[l, 1 + v, r0 : r0 + 16, :] = block
        r, q = iota2(8 * C, C)
        spread = jnp.where(r // 8 == q, 1.0, 0.0).astype(BF)
        nt = (((1,), (1,)), ((), ()))
        half = lax.dot_general(spread, mix_w[l], nt, preferred_element_type=F32).astype(BF)
        full = lax.dot_general(half, spread, nt, preferred_element_type=F32)
        r, q = iota2(8 * C, 8 * C)
        am[l] = jnp.where(r % 8 == q % 8, 0.5 * full, 0.0).astype(BF)
        for d in range(C):
            ab[l, 8 * d : 8 * d + 8, :] = jnp.full((8, 128), 0.5 * bias[l, d], F32)
        return 0

    lax.fori_loop(0, ay.shape[0], layer, 0)


def cost(flops):
    return pl.CostEstimate(flops=flops, bytes_accessed=8 << 20, transcendentals=0)


def params():
    return pltpu.CompilerParams(vmem_limit_bytes=60 << 20)


def relayout_out(vol, xi, shape):
    C, I, J, K = shape
    cb = 4

    def body(xi_ref, v_ref, o_ref):
        flip = xi_ref[0]
        for tp in range(I // 2):
            a = [v_ref[jb, :, 16 * tp : 16 * tp + 16, :].astype(F32) for jb in range(4)]
            for u in range(2):
                t = 2 * tp + u
                b = jnp.concatenate([q[:, 8 * u : 8 * u + 8, :] for q in a], axis=1)
                b = jnp.concatenate([b[:, :, :64], b[:, :, 64:]], axis=1).astype(BF)
                o_ref[:, jnp.where(flip == 1, I - 1 - t, t)] = b

    return pl.pallas_call(
        body,
        grid_spec=pltpu.PrefetchScalarGridSpec(
            num_scalar_prefetch=1,
            grid=(C // cb,),
            in_specs=[pl.BlockSpec((4, cb, I * 8, 128), lambda g, f: (0, g, 0, 0))],
            out_specs=pl.BlockSpec((cb, I, J, K), lambda g, f: (g, 0, 0, 0)),
        ),
        out_shape=jax.ShapeDtypeStruct(shape, BF),
        compiler_params=params(),
        cost_estimate=cost(1 << 26),
        name="relayout_out",
    )(xi, vol)


def x_slab(a, vol, row0, u1, up, dn, C):
    per = X_UNROLL

    def step(it, _):
        low = lane_iota((128, 128)) < 64
        for q in range(per):
            pair = it * per + q
            ends = []
            for c in (2 * pair, 2 * pair + 1):
                got = []
                for jp in range(2):
                    cols = [vol[2 * jp + b, c, pl.ds(row0, 256), :] for b in range(2)]
                    u = jnp.dot(a, jnp.concatenate(cols, axis=1), preferred_element_type=F32)
                    u = u.astype(BF)
                    u1[c, 2 * jp] = u[:, :128]
                    u1[c, 2 * jp + 1] = u[:, 128:]
                    got.append(u[:, :128] if jp == 0 else u[:, 128:])
                ends.append(got)
            up[pair] = jnp.where(low, pltpu.roll(ends[0][1], 64, 1), ends[1][1])
            dn[pair] = jnp.where(low, ends[0][0], pltpu.roll(ends[1][0], 64, 1))
        return 0

    lax.fori_loop(0, C // 2 // per, step, 0)


def y_slab(a, u_ref, b_ref, t_ref, o_ref, up_ref, dn_ref, C):
    def one(pair):
        low = lane_iota((128, 128)) < 64
        slot = (lane_iota((16, 128)) % 64) // 8
        c0, c1 = 2 * pair, 2 * pair + 1
        b, t = b_ref[pair], t_ref[pair]
        first = [u_ref[c, 0] for c in (c0, c1)]
        final = [u_ref[c, 3] for c in (c0, c1)]
        lead = [
            jnp.where(low, b, pltpu.roll(final[0], 64, 1)),
            pltpu.roll(jnp.where(low, final[1], b), 64, 1),
        ]
        tail = [
            pltpu.roll(jnp.where(low, t, first[0]), 64, 1),
            jnp.where(low, pltpu.roll(first[1], 64, 1), t),
        ]
        out_rows = pl.ds(pl.multiple_of(16 * pair, 16), 16)
        for g in range(2):
            rows = slice(64 * g, 64 * g + 64)
            for w in range(2):
                cols = []
                for n, c in enumerate((c0, c1)):
                    own = [u_ref[c, jb, rows, :] for jb in range(1, 3)]
                    if w == 0:
                        blocks = [lead[n][rows], u_ref[c, 0, rows, :]] + own
                    else:
                        blocks = own + [u_ref[c, 3, rows, :], tail[n][rows]]
                    cols.append(jnp.concatenate(blocks, axis=0))
                out = jnp.dot(a, jnp.concatenate(cols, axis=1), preferred_element_type=F32)
                out = out.reshape(2, 8, 8, 256)
                out = jnp.concatenate([out[..., :128], out[..., 128:]], axis=2).astype(BF)
                o_ref[2 * w : 2 * w + 2, 8 * g : 8 * g + 8, out_rows, :] = out
                for e in range(2):
                    up = dn = None
                    for i in range(8):
                        ru = pltpu.roll(out[e, i], (8 * i + 72) % 128, 1)
                        rd = out[e, i] if i == 0 else pltpu.roll(out[e, i], 8 * i, 1)
                        up = ru if up is None else jnp.where(slot == i, ru, up)
                        dn = rd if dn is None else jnp.where(slot == i, rd, dn)
                    up_ref[2 * w + e, g, out_rows, :] = up
                    dn_ref[2 * w + e, g, out_rows, :] = dn

    def step(it, _):
        for q in range(Y_UNROLL):
            one(it * Y_UNROLL + q)
        return 0

    lax.fori_loop(0, C // 2 // Y_UNROLL, step, 0)


def z_slab(z_ref, w_ref, bias_ref, u_ref, b_ref, t_ref, vol, row0, u3_ref, C):
    def z_pair(jb, ip):
        lhs = jnp.concatenate([u_ref[jb, 2 * ip + q, : 8 * C, :] for q in range(2)], axis=1)
        halo = jnp.concatenate([b_ref[jb, ip // 4], t_ref[jb, ip // 4]], axis=1)
        u3 = jnp.dot(lhs, z_ref[0], preferred_element_type=F32)
        u3 = u3 + jnp.dot(halo, z_ref[1 + ip % 4], preferred_element_type=F32)
        return u3.astype(BF)

    u3_ref[...] = z_pair(0, 0)

    def step(jb, _):
        u3 = u3_ref[...]
        for ip in range(8):
            ahead = z_pair(jb, ip + 1) if ip < 7 else z_pair(jnp.minimum(jb + 1, 3), 0)
            bias = bias_ref[...].reshape(C, 8, 128)
            m = jnp.dot(w_ref[...], u3, preferred_element_type=F32).reshape(C, 8, 256)
            m = jnp.concatenate([m[..., :128] + bias, m[..., 128:] + bias], axis=1)
            gelu = m + m * lax.erf(m * SQRT_TWO)
            rows = pl.ds(pl.multiple_of(row0 + 16 * ip, 16), 16)
            v = vol[jb, :, rows, :].astype(F32)
            vol[jb, :, rows, :] = (v + gelu).astype(BF)
            u3 = ahead
        u3_ref[...] = u3
        return 0

    lax.fori_loop(0, 4, step, 0)


def fused_layers(volume, filter_taps, mix_w, mix_bias, ny, nz):
    C, I, J, K = volume.shape
    rows = 8 * I
    L = mix_w.shape[0]
    IN = 4
    S = rows // 128
    N = L * S
    R = 4
    edge = 64 + rows

    def body(vin, taps, wraw, braw, vout, ax, ay, az, am, ab, stage_in, vol, far, u1, u2, u3, ysend, yrecv, zsend, zrecv,
             in_sem, out_sem, far_ss, far_rs, ys_sem, yr_sem, zs_sem, zr_sem):
        xi, yi, zi = (lax.axis_index(a) for a in ("x", "y", "z"))

        def remote(src, dst, ss, rs, axis, idx):
            return pltpu.make_async_remote_copy(
                src_ref=src, dst_ref=dst, send_sem=ss, recv_sem=rs, device_id={axis: idx}, device_id_type=pl.DeviceIdType.MESH
            )

        def ports(axis, pos, count):
            return ((pos < count - 1, pos + 1, pos > 0), (pos > 0, pos - 1, pos < count - 1))

        def link(axis, pos, count, send, recv, ss, rs):
            info = ports(axis, pos, count)

            def copy(d, n):
                a, b = n % 2, n % R
                return remote(send.at[d, a], recv.at[d, b], ss.at[d, a], rs.at[d, b], axis, info[d][1])

            def start(n):
                for d in range(2):
                    @pl.when(info[d][0])
                    def _():
                        copy(d, n).start()

            def wait_send(n):
                for d in range(2):
                    @pl.when(info[d][0])
                    def _():
                        copy(d, n).wait_send()

            def wait_recv(n):
                for d in range(2):
                    @pl.when(info[d][2])
                    def _():
                        copy(d, n).wait_recv()

            return start, wait_send, wait_recv

        y_start, y_wait_send, y_wait_recv = link("y", yi, ny, ysend, yrecv, ys_sem, yr_sem)
        z_start, z_wait_send, z_wait_recv = link("z", zi, nz, zsend, zrecv, zs_sem, zr_sem)

        def far_copy(l):
            a = l % 2
            return remote(vol.at[:, :, pl.ds(edge - 64, 64), :], far.at[a], far_ss.at[a], far_rs.at[a], "x", 1 - xi)

        mirrored = xi == 1

        def in_copy(q):
            at = jnp.where(mirrored, I - 2 - 2 * q, 2 * q)
            return pltpu.make_async_copy(vin.at[:, pl.ds(at, 2)], stage_in.at[q % IN], in_sem.at[q % IN])

        def bring_in(q, _):
            in_copy(q).wait()
            per = 16

            def part(g, _):
                c = pl.ds(per * g, per)
                planes = []
                for u in range(2):
                    a = stage_in[q % IN, c, jnp.where(mirrored, 1 - u, u)].astype(F32)
                    a = jnp.concatenate([a[:, : J // 2], a[:, J // 2 :]], axis=2)
                    planes.append(a.reshape(per, 4, 8, 128))
                both = jnp.concatenate(planes, axis=2).astype(BF)
                at = pl.ds(pl.multiple_of(64 + 16 * q, 16), 16)
                for jb in range(4):
                    vol[jb, c, at, :] = both[:, jb]
                return 0

            lax.fori_loop(0, C // per, part, 0)

            @pl.when(q + IN < I // 2)
            def _():
                in_copy(q + IN).start()

            return 0

        def out_copy(s):
            at = pl.multiple_of(128 * s, 128)
            return pltpu.make_async_copy(vol.at[:, :, pl.ds(64 + at, 128), :], vout.at[:, :, pl.ds(at, 128), :], out_sem.at[s])

        for q in range(IN):
            in_copy(q).start()
        barrier = pltpu.get_barrier_semaphore()
        pl.semaphore_signal(barrier, inc=1, device_id={"x": 1 - xi}, device_id_type=pl.DeviceIdType.MESH)
        for axis, pos, count in (("y", yi, ny), ("z", zi, nz)):
            for ok, idx, _ in ports(axis, pos, count):
                @pl.when(ok)
                def _():
                    pl.semaphore_signal(barrier, inc=1, device_id={axis: idx}, device_id_type=pl.DeviceIdType.MESH)
        greet = 1
        for pos, count in ((yi, ny), (zi, nz)):
            greet = greet + (pos > 0).astype(jnp.int32) + (pos < count - 1).astype(jnp.int32)
        pl.semaphore_wait(barrier, greet)

        def zero_margin(c, _):
            for jb in range(4):
                vol[jb, c, 0:64, :] = jnp.zeros((64, 128), BF)
            return 0

        lax.fori_loop(0, C, zero_margin, 0)
        build_x_tables(taps, ax, mirrored)

        def late_setup():
            for recv, pos, count in ((yrecv, yi, ny), (zrecv, zi, nz)):
                for d, alone in ((0, pos == 0), (1, pos == count - 1)):
                    @pl.when(alone)
                    def _():
                        def zero(r, _):
                            for j in range(recv.shape[2]):
                                recv[d, r, j] = jnp.zeros(recv.shape[3:], BF)
                            return 0

                        lax.fori_loop(0, R, zero, 0)
            build_tables(taps, wraw, braw, ay, az, am, ab)

        def stage(n, _):
            @pl.when(n < N)
            def _():
                l, s = n // S, n % S

                @pl.when(n == 0)
                def _():
                    lax.fori_loop(0, 3 * SLAB // 4, bring_in, 0)

                @pl.when(n == 1)
                def _():
                    lax.fori_loop(3 * SLAB // 4, I // 2, bring_in, 0)
                    far_copy(0).start()
                    late_setup()

                @pl.when(s == S - 1)
                def _():
                    far_copy(l).wait()

                    def bring(c, _):
                        for jb in range(4):
                            vol[jb, c, edge : edge + 64, :] = far[l % 2, jb, c]
                        return 0

                    lax.fori_loop(0, C, bring, 0)

                @pl.when(n >= 2)
                def _():
                    y_wait_send(n - 2)

                a = ax[l, (s == S - 1).astype(jnp.int32)]
                x_slab(a, vol, pl.multiple_of(128 * s, 128), u1.at[n % 2], ysend.at[0, n % 2], ysend.at[1, n % 2], C)
                y_start(n)

            @pl.when((n >= 1) & (n <= N))
            def _():
                m = n - 1
                y_wait_recv(m)

                @pl.when(m >= 2)
                def _():
                    z_wait_send(m - 2)

                y_slab(ay[m // S], u1.at[m % 2], yrecv.at[0, m % R], yrecv.at[1, m % R], u2.at[m % 2],
                       zsend.at[0, m % 2], zsend.at[1, m % 2], C)
                z_start(m)

            @pl.when(n >= 2)
            def _():
                m = n - 2
                l, s = m // S, m % S
                z_wait_recv(m)
                z_slab(az.at[l], am.at[l], ab.at[l], u2.at[m % 2], zrecv.at[0, m % R], zrecv.at[1, m % R], vol,
                       64 + 128 * s, u3, C)

                @pl.when((s == S - 1) & (l < L - 1))
                def _():
                    far_copy(l + 1).start()

                @pl.when(l == L - 1)
                def _():
                    out_copy(s).start()

            return 0

        lax.fori_loop(0, N + 2, stage, 0)
        for n in (N - 2, N - 1):
            y_wait_send(n)
            z_wait_send(n)
        for s in range(S):
            out_copy(s).wait()

    vmem = pl.BlockSpec(memory_space=pltpu.VMEM)
    smem = pl.BlockSpec(memory_space=pltpu.SMEM)
    hbm = pl.BlockSpec(memory_space=pltpu.HBM)
    dma = pltpu.SemaphoreType.DMA
    return pl.pallas_call(
        body,
        in_specs=[hbm, smem, vmem, smem],
        out_specs=hbm,
        out_shape=jax.ShapeDtypeStruct((4, C, rows, 128), BF),
        scratch_shapes=[
            pltpu.VMEM((L, 2, 128, 256), BF),
            pltpu.VMEM((L, 128, 256), BF),
            pltpu.VMEM((L, 5, 256, 256), BF),
            pltpu.VMEM((L, 8 * C, 8 * C), BF),
            pltpu.VMEM((L, 8 * C, 128), F32),
            pltpu.VMEM((IN, C, 2, J, K), BF),
            pltpu.VMEM((4, C, rows + 128, 128), BF),
            pltpu.VMEM((2, 4, C, 64, 128), BF),
            pltpu.VMEM((2, C, 4, 128, 128), BF),
            pltpu.VMEM((2, 4, SLAB, 8 * C, 128), BF),
            pltpu.VMEM((8 * C, 256), BF),
            pltpu.VMEM((2, 2, C // 2, 128, 128), BF),
            pltpu.VMEM((2, R, C // 2, 128, 128), BF),
            pltpu.VMEM((2, 2, 4, 2, 8 * C, 128), BF),
            pltpu.VMEM((2, R, 4, 2, 8 * C, 128), BF),
            dma((IN,)),
            dma((S,)),
            dma((2,)),
            dma((2,)),
            dma((2, 2)),
            dma((2, R)),
            dma((2, 2)),
            dma((2, R)),
        ],
        compiler_params=pltpu.CompilerParams(vmem_limit_bytes=67043328, collective_id=0, has_side_effects=True),
        cost_estimate=cost(1 << 32),
        name="fused_layers",
    )(volume, filter_taps.reshape(-1, filter_taps.shape[2]), mix_w, mix_bias)


def solution(mesh):
    ny, nz = mesh.shape["y"], mesh.shape["z"]

    def local_layers(volume, filter_taps, mix_w, mix_bias):
        xi = lax.axis_index("x").astype(jnp.int32)
        xi_arr = xi.reshape(1)
        out = fused_layers(volume, filter_taps, mix_w, mix_bias, ny, nz)
        return relayout_out(out, xi_arr, volume.shape)

    vol_spec = P("batch", "x", "y", "z")
    return jax.shard_map(
        local_layers, mesh=mesh, in_specs=(vol_spec, P(), P(), P()), out_specs=vol_spec, check_vma=False
    )
```

```python
import jax
import jax.numpy as jnp
from jax import lax
from jax.experimental import pallas as pl
from jax.experimental.pallas import tpu as pltpu
from jax.sharding import PartitionSpec as P

BF = jnp.bfloat16
F32 = jnp.float32
SLAB = 16
X_UNROLL, Y_UNROLL = 16, 4
Z_UNROLL, Z_AHEAD = 2, 2
JH = 2
SQRT_TWO = 1.4142135623730951


def lane_iota(shape):
    return lax.broadcasted_iota(jnp.int32, shape, len(shape) - 1)


def iota2(rows, cols, row0=0):
    return lax.broadcasted_iota(jnp.int32, (rows, cols), 0) + row0, lax.broadcasted_iota(jnp.int32, (rows, cols), 1)


def tap_values(taps, row, index, valid, mirrored=None):
    index = jnp.where(valid, index, -1)
    count = taps.shape[1]
    out = jnp.zeros(index.shape, F32)
    for t in range(count):
        src = t if mirrored is None else jnp.where(mirrored, count - 1 - t, t)
        out = jnp.where(index == t, taps[row, src], out)
    return out


def build_x_tables(taps, ax, mirrored):
    span = taps.shape[1]

    def layer(l, _):
        for last in range(2):
            for r0 in range(0, 128, 32):
                r, q = iota2(32, 256, r0)
                i_in = q // 8
                if last:
                    i_in = jnp.where(i_in >= 24, 55 - i_in, i_in)
                t = i_in - r // 8
                ok = (t >= 0) & (t < span) & (r % 8 == q % 8)
                ax[l, last, r0 : r0 + 32, :] = tap_values(taps, 3 * l, t, ok, mirrored).astype(BF)
        return 0

    lax.fori_loop(0, ax.shape[0], layer, 0)


def build_tables(taps, mix_w, bias, ay, az, am, ab):
    C = mix_w.shape[1]
    span = taps.shape[1]

    def layer(l, _):
        for r0 in range(0, 128, 32):
            r, q = iota2(32, 256, r0)
            t = (q // 64) * 8 + q % 8 - (r // 64) * 8 - r % 8
            ok = (t >= 0) & (t < span) & ((r // 8) % 8 == (q // 8) % 8)
            ay[l, r0 : r0 + 32, :] = tap_values(taps, 3 * l + 1, t, ok).astype(BF)
        for k0 in range(0, 64, 32):
            k, n = iota2(32, 256, k0)
            t = k - n % 64 + 8
            base = tap_values(taps, 3 * l + 2, t, (t >= 0) & (t < span))
            for g in range(4):
                az[l, 0, 64 * g + k0 : 64 * g + k0 + 32, :] = jnp.where(n // 64 == g, base, 0.0).astype(BF)
        for v in range(4):
            for r0 in range(0, 256, 64):
                az[l, 1 + v, r0 : r0 + 64, :] = jnp.zeros((64, 256), BF)
        r, n = iota2(16, 256)
        for side in range(2):
            t = r % 8 - n % 64 + 72 * side
            base = tap_values(taps, 3 * l + 2, t, (t >= 0) & (t < span) & (r // 8 == n // 128))
            for jh in range(2):
                block = jnp.where((n // 64) % 2 == jh, base, 0.0).astype(BF)
                for v in range(4):
                    r0 = 128 * side + 64 * jh + 16 * v
                    az[l, 1 + v, r0 : r0 + 16, :] = block
        r, q = iota2(8 * C, C)
        spread = jnp.where(r // 8 == q, 1.0, 0.0).astype(BF)
        nt = (((1,), (1,)), ((), ()))
        half = lax.dot_general(spread, mix_w[l], nt, preferred_element_type=F32).astype(BF)
        full = lax.dot_general(half, spread, nt, preferred_element_type=F32)
        r, q = iota2(8 * C, 8 * C)
        am[l] = jnp.where(r % 8 == q % 8, 0.5 * full, 0.0).astype(BF)
        for d in range(C):
            ab[l, 8 * d : 8 * d + 8, :] = jnp.full((8, 128), 0.5 * bias[l, d], F32)
        return 0

    lax.fori_loop(0, ay.shape[0], layer, 0)


def cost(flops):
    return pl.CostEstimate(flops=flops, bytes_accessed=8 << 20, transcendentals=0)


def params():
    return pltpu.CompilerParams(vmem_limit_bytes=60 << 20)


def relayout_out(vol, xi, shape):
    C, I, J, K = shape
    cb = 4

    def body(xi_ref, v_ref, o_ref):
        flip = xi_ref[0]
        for tp in range(I // 2):
            a = [v_ref[jb, :, 16 * tp : 16 * tp + 16, :].astype(F32) for jb in range(4)]
            for u in range(2):
                t = 2 * tp + u
                b = jnp.concatenate([q[:, 8 * u : 8 * u + 8, :] for q in a], axis=1)
                b = jnp.concatenate([b[:, :, :64], b[:, :, 64:]], axis=1).astype(BF)
                o_ref[:, jnp.where(flip == 1, I - 1 - t, t)] = b

    return pl.pallas_call(
        body,
        grid_spec=pltpu.PrefetchScalarGridSpec(
            num_scalar_prefetch=1,
            grid=(C // cb,),
            in_specs=[pl.BlockSpec((4, cb, I * 8, 128), lambda g, f: (0, g, 0, 0))],
            out_specs=pl.BlockSpec((cb, I, J, K), lambda g, f: (g, 0, 0, 0)),
        ),
        out_shape=jax.ShapeDtypeStruct(shape, BF),
        compiler_params=params(),
        cost_estimate=cost(1 << 26),
        name="relayout_out",
    )(xi, vol)


def x_slab(a, vol, row0, u1, up, dn, C):
    per = X_UNROLL

    def step(it, _):
        low = lane_iota((128, 128)) < 64
        for q in range(per):
            pair = it * per + q
            ends = []
            for c in (2 * pair, 2 * pair + 1):
                got = []
                for jp in range(2):
                    cols = [vol[2 * jp + b, c, pl.ds(row0, 256), :] for b in range(2)]
                    u = jnp.dot(a, jnp.concatenate(cols, axis=1), preferred_element_type=F32)
                    u = u.astype(BF)
                    u1[c, 2 * jp] = u[:, :128]
                    u1[c, 2 * jp + 1] = u[:, 128:]
                    got.append(u[:, :128] if jp == 0 else u[:, 128:])
                ends.append(got)
            up[pair] = jnp.where(low, pltpu.roll(ends[0][1], 64, 1), ends[1][1])
            dn[pair] = jnp.where(low, ends[0][0], pltpu.roll(ends[1][0], 64, 1))
        return 0

    lax.fori_loop(0, C // 2 // per, step, 0)


def y_slab(a, u_ref, b_ref, t_ref, o_ref, up_ref, dn_ref, C):
    def one(pair):
        low = lane_iota((128, 128)) < 64
        slot = (lane_iota((16, 128)) % 64) // 8
        c0, c1 = 2 * pair, 2 * pair + 1
        b, t = b_ref[pair], t_ref[pair]
        first = [u_ref[c, 0] for c in (c0, c1)]
        final = [u_ref[c, 3] for c in (c0, c1)]
        lead = [
            jnp.where(low, b, pltpu.roll(final[0], 64, 1)),
            pltpu.roll(jnp.where(low, final[1], b), 64, 1),
        ]
        tail = [
            pltpu.roll(jnp.where(low, t, first[0]), 64, 1),
            jnp.where(low, pltpu.roll(first[1], 64, 1), t),
        ]
        out_rows = pl.ds(pl.multiple_of(16 * pair, 16), 16)
        for g in range(2):
            rows = slice(64 * g, 64 * g + 64)
            for w in range(2):
                cols = []
                for n, c in enumerate((c0, c1)):
                    own = [u_ref[c, jb, rows, :] for jb in range(1, 3)]
                    if w == 0:
                        blocks = [lead[n][rows], u_ref[c, 0, rows, :]] + own
                    else:
                        blocks = own + [u_ref[c, 3, rows, :], tail[n][rows]]
                    cols.append(jnp.concatenate(blocks, axis=0))
                out = jnp.dot(a, jnp.concatenate(cols, axis=1), preferred_element_type=F32)
                out = out.reshape(2, 8, 8, 256)
                out = jnp.concatenate([out[..., :128], out[..., 128:]], axis=2).astype(BF)
                o_ref[2 * w : 2 * w + 2, 8 * g : 8 * g + 8, out_rows, :] = out
                for e in range(2):
                    up = dn = None
                    for i in range(8):
                        ru = pltpu.roll(out[e, i], (8 * i + 72) % 128, 1)
                        rd = out[e, i] if i == 0 else pltpu.roll(out[e, i], 8 * i, 1)
                        up = ru if up is None else jnp.where(slot == i, ru, up)
                        dn = rd if dn is None else jnp.where(slot == i, rd, dn)
                    up_ref[2 * w + e, g, out_rows, :] = up
                    dn_ref[2 * w + e, g, out_rows, :] = dn

    def step(it, _):
        for q in range(Y_UNROLL):
            one(it * Y_UNROLL + q)
        return 0

    lax.fori_loop(0, C // 2 // Y_UNROLL, step, 0)


def z_slab(z_ref, w_ref, bias_ref, u_ref, b_ref, t_ref, vol, row0, u3_ref, C):
    def z_pair(jb, ip):
        lhs = jnp.concatenate([u_ref[jb, 2 * ip + q, : 8 * C, :] for q in range(2)], axis=1)
        halo = jnp.concatenate([b_ref[jb, ip // 4], t_ref[jb, ip // 4]], axis=1)
        u3 = jnp.dot(lhs, z_ref[0], preferred_element_type=F32)
        u3 = u3 + jnp.dot(halo, z_ref[1 + ip % 4], preferred_element_type=F32)
        return u3.astype(BF)

    for q in range(Z_AHEAD):
        u3_ref[q] = z_pair(0, q)

    def step(it, _):
        u3 = [u3_ref[q] for q in range(Z_AHEAD)]
        for q in range(8 * Z_UNROLL):
            jb, ip, nxt = it * Z_UNROLL + q // 8, q % 8, q % 8 + Z_AHEAD
            u3.append(z_pair(jnp.minimum(jb + nxt // 8, 3), nxt % 8))
            bias = bias_ref[...].reshape(C, 8, 128)
            m = jnp.dot(w_ref[...], u3[q], preferred_element_type=F32).reshape(C, 8, 256)
            m = jnp.concatenate([m[..., :128] + bias, m[..., 128:] + bias], axis=1)
            gelu = m + m * lax.erf(m * SQRT_TWO)
            rows = pl.ds(pl.multiple_of(row0 + 16 * ip, 16), 16)
            v = vol[jb, :, rows, :].astype(F32)
            vol[jb, :, rows, :] = (v + gelu).astype(BF)
        for q in range(Z_AHEAD):
            u3_ref[q] = u3[8 * Z_UNROLL + q]
        return 0

    lax.fori_loop(0, 4 // Z_UNROLL, step, 0)


def fused_layers(volume, filter_taps, mix_w, mix_bias, ny, nz):
    C, I, J, K = volume.shape
    rows = 8 * I
    L = mix_w.shape[0]
    IN = 4
    S = rows // 128
    N = L * S
    R = 4
    edge = 64 + rows

    def body(vin, taps, wraw, braw, vout, ax, ay, az, am, ab, stage_in, vol, far, u1, u2, u3, ysend, yrecv, zsend, zrecv,
             in_sem, out_sem, far_ss, far_rs, ys_sem, yr_sem, zs_sem, zr_sem):
        xi, yi, zi = (lax.axis_index(a) for a in ("x", "y", "z"))

        def remote(src, dst, ss, rs, axis, idx):
            return pltpu.make_async_remote_copy(
                src_ref=src, dst_ref=dst, send_sem=ss, recv_sem=rs, device_id={axis: idx}, device_id_type=pl.DeviceIdType.MESH
            )

        def ports(axis, pos, count):
            return ((pos < count - 1, pos + 1, pos > 0), (pos > 0, pos - 1, pos < count - 1))

        def link(axis, pos, count, send, recv, ss, rs):
            info = ports(axis, pos, count)

            def copy(d, n):
                a, b = n % 2, n % R
                return remote(send.at[d, a], recv.at[d, b], ss.at[d, a], rs.at[d, b], axis, info[d][1])

            def start(n):
                for d in range(2):
                    @pl.when(info[d][0])
                    def _():
                        copy(d, n).start()

            def wait_send(n):
                for d in range(2):
                    @pl.when(info[d][0])
                    def _():
                        copy(d, n).wait_send()

            def wait_recv(n):
                for d in range(2):
                    @pl.when(info[d][2])
                    def _():
                        copy(d, n).wait_recv()

            return start, wait_send, wait_recv

        y_start, y_wait_send, y_wait_recv = link("y", yi, ny, ysend, yrecv, ys_sem, yr_sem)
        z_start, z_wait_send, z_wait_recv = link("z", zi, nz, zsend, zrecv, zs_sem, zr_sem)

        def far_copy(l):
            a = l % 2
            return remote(vol.at[:, :, pl.ds(edge - 64, 64), :], far.at[a], far_ss.at[a], far_rs.at[a], "x", 1 - xi)

        mirrored = xi == 1

        def in_copy(q):
            at = jnp.where(mirrored, I - 2 - 2 * q, 2 * q)
            return pltpu.make_async_copy(vin.at[:, pl.ds(at, 2)], stage_in.at[q % IN], in_sem.at[q % IN])

        def bring_in(q, _):
            in_copy(q).wait()
            per = 16

            def part(g, _):
                c = pl.ds(per * g, per)
                planes = []
                for u in range(2):
                    a = stage_in[q % IN, c, jnp.where(mirrored, 1 - u, u)].astype(F32)
                    a = jnp.concatenate([a[:, : J // 2], a[:, J // 2 :]], axis=2)
                    planes.append(a.reshape(per, 4, 8, 128))
                both = jnp.concatenate(planes, axis=2).astype(BF)
                at = pl.ds(pl.multiple_of(64 + 16 * q, 16), 16)
                for jb in range(4):
                    vol[jb, c, at, :] = both[:, jb]
                return 0

            lax.fori_loop(0, C // per, part, 0)

            @pl.when(q + IN < I // 2)
            def _():
                in_copy(q + IN).start()

            return 0

        def out_copy(s):
            at = pl.multiple_of(128 * s, 128)
            return pltpu.make_async_copy(vol.at[:, :, pl.ds(64 + at, 128), :], vout.at[:, :, pl.ds(at, 128), :], out_sem.at[s])

        for q in range(IN):
            in_copy(q).start()
        barrier = pltpu.get_barrier_semaphore()
        pl.semaphore_signal(barrier, inc=1, device_id={"x": 1 - xi}, device_id_type=pl.DeviceIdType.MESH)
        for axis, pos, count in (("y", yi, ny), ("z", zi, nz)):
            for ok, idx, _ in ports(axis, pos, count):
                @pl.when(ok)
                def _():
                    pl.semaphore_signal(barrier, inc=1, device_id={axis: idx}, device_id_type=pl.DeviceIdType.MESH)
        greet = 1
        for pos, count in ((yi, ny), (zi, nz)):
            greet = greet + (pos > 0).astype(jnp.int32) + (pos < count - 1).astype(jnp.int32)
        pl.semaphore_wait(barrier, greet)

        def zero_margin(c, _):
            for jb in range(4):
                vol[jb, c, 0:64, :] = jnp.zeros((64, 128), BF)
            return 0

        lax.fori_loop(0, C, zero_margin, 0)
        build_x_tables(taps, ax, mirrored)

        def late_setup():
            for recv, pos, count in ((yrecv, yi, ny), (zrecv, zi, nz)):
                for d, alone in ((0, pos == 0), (1, pos == count - 1)):
                    @pl.when(alone)
                    def _():
                        def zero(r, _):
                            for j in range(recv.shape[2]):
                                recv[d, r, j] = jnp.zeros(recv.shape[3:], BF)
                            return 0

                        lax.fori_loop(0, R, zero, 0)
            build_tables(taps, wraw, braw, ay, az, am, ab)

        def stage(n, _):
            @pl.when(n < N)
            def _():
                l, s = n // S, n % S

                @pl.when(n == 0)
                def _():
                    lax.fori_loop(0, 3 * SLAB // 4, bring_in, 0)

                @pl.when(n == 1)
                def _():
                    lax.fori_loop(3 * SLAB // 4, I // 2, bring_in, 0)
                    far_copy(0).start()
                    late_setup()

                @pl.when(s == S - 1)
                def _():
                    far_copy(l).wait()

                    def bring(c, _):
                        for jb in range(4):
                            vol[jb, c, edge : edge + 64, :] = far[l % 2, jb, c]
                        return 0

                    lax.fori_loop(0, C, bring, 0)

                @pl.when(n >= 2)
                def _():
                    y_wait_send(n - 2)

                a = ax[l, (s == S - 1).astype(jnp.int32)]
                x_slab(a, vol, pl.multiple_of(128 * s, 128), u1.at[n % 2], ysend.at[0, n % 2], ysend.at[1, n % 2], C)
                y_start(n)

            @pl.when((n >= 1) & (n <= N))
            def _():
                m = n - 1
                y_wait_recv(m)

                @pl.when(m >= 2)
                def _():
                    z_wait_send(m - 2)

                y_slab(ay[m // S], u1.at[m % 2], yrecv.at[0, m % R], yrecv.at[1, m % R], u2.at[m % 2],
                       zsend.at[0, m % 2], zsend.at[1, m % 2], C)
                z_start(m)

            @pl.when(n >= 2)
            def _():
                m = n - 2
                l, s = m // S, m % S
                z_wait_recv(m)
                z_slab(az.at[l], am.at[l], ab.at[l], u2.at[m % 2], zrecv.at[0, m % R], zrecv.at[1, m % R], vol,
                       64 + 128 * s, u3, C)

                @pl.when((s == S - 1) & (l < L - 1))
                def _():
                    far_copy(l + 1).start()

                @pl.when(l == L - 1)
                def _():
                    out_copy(s).start()

            return 0

        lax.fori_loop(0, N + 2, stage, 0)
        for n in (N - 2, N - 1):
            y_wait_send(n)
            z_wait_send(n)
        for s in range(S):
            out_copy(s).wait()

    vmem = pl.BlockSpec(memory_space=pltpu.VMEM)
    smem = pl.BlockSpec(memory_space=pltpu.SMEM)
    hbm = pl.BlockSpec(memory_space=pltpu.HBM)
    dma = pltpu.SemaphoreType.DMA
    return pl.pallas_call(
        body,
        in_specs=[hbm, smem, vmem, smem],
        out_specs=hbm,
        out_shape=jax.ShapeDtypeStruct((4, C, rows, 128), BF),
        scratch_shapes=[
            pltpu.VMEM((L, 2, 128, 256), BF),
            pltpu.VMEM((L, 128, 256), BF),
            pltpu.VMEM((L, 5, 256, 256), BF),
            pltpu.VMEM((L, 8 * C, 8 * C), BF),
            pltpu.VMEM((L, 8 * C, 128), F32),
            pltpu.VMEM((IN, C, 2, J, K), BF),
            pltpu.VMEM((4, C, rows + 128, 128), BF),
            pltpu.VMEM((2, 4, C, 64, 128), BF),
            pltpu.VMEM((2, C, 4, 128, 128), BF),
            pltpu.VMEM((2, 4, SLAB, 8 * C, 128), BF),
            pltpu.VMEM((Z_AHEAD, 8 * C, 256), BF),
            pltpu.VMEM((2, 2, C // 2, 128, 128), BF),
            pltpu.VMEM((2, R, C // 2, 128, 128), BF),
            pltpu.VMEM((2, 2, 4, 2, 8 * C, 128), BF),
            pltpu.VMEM((2, R, 4, 2, 8 * C, 128), BF),
            dma((IN,)),
            dma((S,)),
            dma((2,)),
            dma((2,)),
            dma((2, 2)),
            dma((2, R)),
            dma((2, 2)),
            dma((2, R)),
        ],
        compiler_params=pltpu.CompilerParams(vmem_limit_bytes=67043328, collective_id=0, has_side_effects=True),
        cost_estimate=cost(1 << 32),
        name="fused_layers",
    )(volume, filter_taps.reshape(-1, filter_taps.shape[2]), mix_w, mix_bias)


def solution(mesh):
    ny, nz = mesh.shape["y"], mesh.shape["z"]

    def local_layers(volume, filter_taps, mix_w, mix_bias):
        xi = lax.axis_index("x").astype(jnp.int32)
        xi_arr = xi.reshape(1)
        out = fused_layers(volume, filter_taps, mix_w, mix_bias, ny, nz)
        return relayout_out(out, xi_arr, volume.shape)

    vol_spec = P("batch", "x", "y", "z")
    return jax.shard_map(
        local_layers, mesh=mesh, in_specs=(vol_spec, P(), P(), P()), out_specs=vol_spec, check_vma=False
    )
```
